32 devices in a mesh: dp: 4 (over z), expert: 8 (over y, x, core).
Axes of the slice: x: 2, y: 2, z: 4, core: 2. Of those that a mesh axis runs over, the one named last changes fastest.
Arguments:
- tokens: bfloat16 [4096, 2048], P(('dp', 'expert')), may hold values from -6 to 6
- cotangent: bfloat16 [4096, 2048], P(('dp', 'expert')), may hold values from -12 to 12
- expert_ids: int32 [4096, 2], P(('dp', 'expert')), may hold values from 0 to 7, all different within a row; in each aligned block of 128 rows (0 to 127, 128 to 255, ...) at most 36 rows name the same one
- router_logits: float32 [4096, 2], P(('dp', 'expert')), may hold values from -6 to 6
- gate_mean: bfloat16 [57344, 2048], P('expert', 'dp'), may hold values from -0.125 to 0.125
- down_mean: bfloat16 [57344, 2048], P('expert', 'dp'), may hold values from -0.0625 to 0.0625
- gate_noise: bfloat16 [57344, 2048], P('expert'), may hold values from -0.0625 to 0.0625
- down_noise: bfloat16 [57344, 2048], P('expert'), may hold values from -0.03125 to 0.03125
Outputs:
- mixed: bfloat16 [4096, 2048], P(('dp', 'expert'))
- precision_down: float32 [2048, 57344], P('dp', 'expert')
The draws below stay inside these ranges and needn't reach their ends.
Inputs may be any that keep to these rules, and one draw needn't show every extreme that they name: `expert_ids`: the 2 experts of a token differ. Among the 128 tokens of one device no expert is named more than 36 times, and some device names some expert exactly 36 times.
All inputs are finite; a program needn't handle non-finite values.
Results may differ from the reference program's by a relative error of at most 0.01.
Values may be sent and summed in bfloat16 or wider, within the bound.
No kernel may reach another device: no remote copies, remote signals or barrier semaphores. Data moves between devices by JAX's collectives and lax.ppermute only.
A program may use at most 256 MiB of HBM per device.

```python
import math
import jax
import jax.numpy as jnp
import numpy as np

D = 2048
FF = 7168
E = 8
TOPK = 2
TOK_DEV = 128
CAP = 36
SLICES = 1
TOKENS = 4096
N_DP = 4
N_EXPERT = 8


def shard_levels(stream_key, extent, split, least, top_value):
    def one(dim, parts):
        draws = jax.random.uniform(jax.random.fold_in(jax.random.fold_in(stream_key, 6), dim), (parts,), jnp.float32, least / len(split), top_value / len(split))
        return jnp.repeat(jnp.exp(draws), extent[dim] // parts).reshape((-1,) + (1,) * (len(extent) - dim - 1))

    loudness = one(*split[0])
    for cut in split[1:]:
        loudness = loudness * one(*cut)
    return loudness


def assign_block(key, own, number, rows, amount, top, limit, slope):
    sequence = jax.random.permutation(key, amount)
    packed, usual = load_shares(amount, rows * top, limit, slope, True), load_shares(amount, rows * top, limit, slope, False)
    places = jnp.arange(amount)

    def named(tallies, offset_by):
        used = int((tallies > 0).sum())
        fixed = max(1, used // 4)
        passed = fixed + (places - fixed + offset_by * (used - fixed)) % max(1, amount - fixed)
        return jnp.zeros((amount,), jnp.int32).at[sequence[jnp.where(places < fixed, places, passed)]].set(jnp.asarray(tallies, jnp.int32))

    tallies = jnp.where(number % 4 == 0, named(packed, number // 4), named(usual, number - number // 4 - 1))
    mixed = jax.random.permutation(jax.random.fold_in(own, 3), amount)
    giver, receiver = mixed[0:amount // 2 * 2:2], mixed[1:amount // 2 * 2:2]
    margin = jnp.minimum(tallies[giver] - 1, limit - tallies[receiver]) // 2
    margin = jnp.where((giver == sequence[0]) | (receiver == sequence[0]) | (tallies[receiver] == 0), 0, jnp.maximum(margin, 0))
    passed = jax.random.randint(jax.random.fold_in(own, 4), (amount // 2,), 0, 1 << 20) % (margin + 1)
    tallies = tallies.at[giver].add(-passed).at[receiver].add(passed)
    items = jnp.searchsorted(jnp.cumsum(tallies), jnp.arange(rows * top), side="right").astype(jnp.int32)
    listing = items.reshape(top, rows).T
    listing = listing[jax.random.permutation(jax.random.fold_in(own, 1), rows)]
    offset_by = jax.random.randint(jax.random.fold_in(own, 2), (rows, 1), 0, top)
    return jnp.take_along_axis(listing, (jnp.arange(top)[None, :] + offset_by) % top, axis=1)


def load_shares(number_of, total, most, slope, full):
    weights = [(1 << 20) // math.isqrt(standing ** slope) + 1 for standing in range(1, number_of + 1)]
    largest = most if full else min(most, max(-(-total // number_of), total * weights[0] // sum(weights)))
    least = 1 if total - largest >= number_of - 1 else 0
    counts, surplus = [largest] + [least] * (number_of - 1), total - largest - least * (number_of - 1)
    while surplus > 0:
        free = [i for i in range(1, number_of) if counts[i] < largest] or [i for i in range(1, number_of) if counts[i] < most]
        whole, left = sum([weights[i] for i in free]), surplus
        for i in free:
            extra = min(most - counts[i], max(1, left * weights[i] // whole), surplus)
            counts[i] = counts[i] + extra
            surplus = surplus - extra
    return np.array(counts)


def gaussian(rng, dims, deviation, limit, cuts=(), held_as=jnp.bfloat16):
    array = deviation * jax.random.normal(rng, dims, jnp.float32)
    if cuts:
        array = array * shard_levels(rng, dims, cuts, -0.22, 0.18)
    return jnp.clip(array, -limit, limit).astype(held_as)


def setup_inputs(seed: int = 0) -> dict:
    key_list = jax.random.split(jax.random.key(seed), 9)
    tokens = gaussian(key_list[0], (TOKENS, D), 1.0, 6.0, ((0, 32),))
    cotangent = gaussian(key_list[1], (TOKENS, D), 2.0, 12.0, ((0, 32),))
    expert_ids_keys = jax.random.split(jax.random.fold_in(key_list[2], 1), TOKENS // TOK_DEV)
    expert_ids_turns = jax.random.permutation(jax.random.fold_in(key_list[2], 3), TOKENS // TOK_DEV)
    expert_ids = jax.vmap(lambda own, number: assign_block(jax.random.fold_in(key_list[2], 2), own, number, TOK_DEV, E, TOPK, CAP, 1))(expert_ids_keys, expert_ids_turns).reshape((TOKENS, TOPK))
    router_logits = gaussian(key_list[3], (TOKENS, TOPK), 1.0, 6.0, ((0, 32),), jnp.float32)
    gate_mean = gaussian(key_list[4], (E * FF, D), D ** -0.5, 0.125, ((0, 8), (1, 4)))
    down_mean = gaussian(key_list[5], (E * FF, D), FF ** -0.5, 0.0625, ((0, 8), (1, 4)))
    gate_noise = gaussian(key_list[6], (E * FF, D), (4 * D) ** -0.5, 0.0625, ((0, 8),))
    down_noise = gaussian(key_list[7], (E * FF, D), (4 * FF) ** -0.5, 0.03125, ((0, 8),))
    return {"tokens": tokens, "cotangent": cotangent, "expert_ids": expert_ids, "router_logits": router_logits, "gate_mean": gate_mean, "down_mean": down_mean, "gate_noise": gate_noise, "down_noise": down_noise}


def silu_of(values):
    return values / (1.0 + jnp.exp(-values))


def reference(tokens, cotangent, expert_ids, router_logits, gate_mean, down_mean, gate_noise, down_noise):
    gate_weight = (gate_mean.astype(jnp.float32) + gate_noise.astype(jnp.float32)).astype(jnp.bfloat16)
    down_weight = (down_mean.astype(jnp.float32) + down_noise.astype(jnp.float32)).astype(jnp.bfloat16)
    mixing = 1.0 / (1.0 + jnp.exp(router_logits[:, ::-1] - router_logits))
    scaled = (mixing[:, :, None] * cotangent.astype(jnp.float32)[:, None, :]).astype(jnp.bfloat16)
    scaled = scaled.reshape(TOKENS * TOPK, D)
    flat_ids = expert_ids.reshape(TOKENS * TOPK).astype(jnp.int32)
    most_rows = N_DP * N_EXPERT * CAP
    slice_width = FF // SLICES
    outputs = jnp.zeros((TOKENS * TOPK, D), jnp.float32)
    precision_cols = []
    for expert in range(E):
        ranked = jnp.argsort((flat_ids != expert).astype(jnp.int32), stable=True)[:most_rows].astype(jnp.int32)
        loaded = jnp.sum((flat_ids == expert).astype(jnp.int32))
        filled = jnp.arange(most_rows, dtype=jnp.int32) < loaded
        token_rows = jnp.where(filled[:, None], tokens[ranked // TOPK], jnp.zeros((), jnp.bfloat16)).astype(jnp.bfloat16)
        scaled_rows = jnp.where(filled[:, None], scaled[ranked], jnp.zeros((), jnp.bfloat16)).astype(jnp.bfloat16)
        gate_rows = gate_weight[expert * FF:(expert + 1) * FF]
        pre_act = jnp.dot(token_rows, gate_rows.T, preferred_element_type=jnp.float32)
        hidden = silu_of(pre_act).astype(jnp.bfloat16)
        summed = jnp.zeros((most_rows, D), jnp.float32)
        for slice_index in range(SLICES):
            first_unit = slice_index * slice_width
            down_rows = down_weight[expert * FF + first_unit:expert * FF + first_unit + slice_width]
            piece_out = jnp.dot(hidden[:, first_unit:first_unit + slice_width], down_rows, preferred_element_type=jnp.float32)
            summed = summed + piece_out.astype(jnp.bfloat16).astype(jnp.float32)
        summed = jnp.where(filled[:, None], summed, jnp.zeros((), jnp.float32))
        outputs = outputs.at[ranked].add(summed)
        hidden_sq = jnp.square(hidden.astype(jnp.float32)).astype(jnp.bfloat16)
        scaled_sq = jnp.square(scaled_rows.astype(jnp.float32)).astype(jnp.bfloat16)
        block_sum = jnp.dot(scaled_sq.T, hidden_sq, preferred_element_type=jnp.float32)
        precision_cols.append(block_sum * (E / TOKENS))
    per_assign = outputs.reshape(TOKENS, TOPK, D)
    mixed = jnp.sum(mixing[:, :, None] * per_assign, axis=1).astype(jnp.bfloat16)
    precision_down = jnp.concatenate(precision_cols, axis=1)
    return mixed, precision_down
```

```python
import jax
import jax.numpy as jnp
from jax import lax
from jax.experimental import pallas as pl
from jax.experimental.pallas import tpu as pltpu
from jax.sharding import PartitionSpec as P

E = 8
TOPK = 2
CAP = 36
CUTS = (2, 2, 2, 2, 2, 2, 1, 1)
VMEM = 60 * 1024 * 1024


def silu_of(values):
    return values / (1.0 + jnp.exp(-values))


def chunk_body(n, h, cols, blocks, factor, first, last, where_ref, *refs):
    gate = refs[:n]
    down = refs[n:n + h]
    g_noise, d_noise, tok_ref, ssq_ref = refs[n + h:n + h + 4]
    acc_in = None if first else refs[n + h + 4]
    refs = refs[n + h + (4 if first else 6):]
    acc_out, out, sent, w, dw, hsq, ssq, acc, held, acc_sem, ssq_sem = refs
    rows = tok_ref.shape[0] // blocks
    step = pl.program_id(0)
    ssq_load = pltpu.make_async_copy(ssq_ref, ssq, ssq_sem)
    if not first:
        acc_load = pltpu.make_async_copy(acc_in, acc, acc_sem)

    @pl.when(step == 0)
    def _():
        if first:
            acc[...] = jnp.zeros_like(acc)
        else:
            acc_load.start()
        ssq_load.start()

    for p in range(n):
        at = pl.ds(pl.multiple_of(where_ref[p] * cols, cols), cols)
        w[:, p * cols:(p + 1) * cols] = gate[p][...] + g_noise[:, at]
        if p < h:
            dw[:, p * cols:(p + 1) * cols] = down[p][...] + d_noise[:, at]

    if not first:
        @pl.when(step == 0)
        def _():
            acc_load.wait()

    for r in range(blocks):
        at = slice(r * rows, (r + 1) * rows)
        pre = lax.dot_general(
            tok_ref[at, :], w[...], (((1,), (1,)), ((), ())), preferred_element_type=jnp.float32
        )
        hidden = silu_of(pre).astype(jnp.bfloat16)
        hsq[at, :] = jnp.square(hidden.astype(jnp.float32)).astype(jnp.bfloat16)
        acc[at, :] += jnp.dot(hidden, dw[...], preferred_element_type=jnp.float32)

    done = step == pl.num_programs(0) - 1
    if last:
        acc_store = pltpu.make_async_copy(held, acc_out, acc_sem)
    else:
        acc_store = pltpu.make_async_copy(acc, acc_out, acc_sem)

    @pl.when(done)
    def _():
        if last:
            held[...] = acc[...].astype(held.dtype)
        acc_store.start()

    @pl.when(step == 0)
    def _():
        ssq_load.wait()

    sent[...] = (
        factor
        * jnp.dot(ssq[: (h - 1) * cols, :], hsq[...], preferred_element_type=jnp.float32)
    ).astype(jnp.bfloat16)
    out[...] = factor * jnp.dot(
        ssq[(h - 1) * cols:, :], hsq[...], preferred_element_type=jnp.float32
    )

    @pl.when(done)
    def _():
        acc_store.wait()


def chunk_call(
    n, h, lo, length, units, factor, where, gate, down, g_noise, d_noise, tok, ssq, acc, out
):
    cols = gate[0].shape[1]
    rows = tok.shape[0]
    first, last = acc is None, lo + length == units
    tile = 512 if length % 512 == 0 else length
    start = lo // tile
    blocks = 3 if rows % 24 == 0 else 1
    mean_spec = pl.BlockSpec((tile, cols), lambda i, s: (i, 0))
    noise_spec = pl.BlockSpec((tile, n * cols), lambda i, s: (start + i, 0))
    any_space = pl.BlockSpec(memory_space=pl.ANY)
    acc_shape = jax.ShapeDtypeStruct((rows, h * cols), jnp.bfloat16 if last else jnp.float32)
    carried = () if first else (acc, out)
    aliases = {} if first else {n + h + 6: 1}
    if not (first or last):
        aliases[n + h + 5] = 0

    def kernel(*refs):
        return chunk_body(n, h, cols, blocks, factor, first, last, *refs)

    return pl.pallas_call(
        kernel,
        grid_spec=pltpu.PrefetchScalarGridSpec(
            num_scalar_prefetch=1,
            grid=(length // tile,),
            in_specs=[mean_spec] * (n + h)
            + [noise_spec, noise_spec]
            + [pl.BlockSpec(tok.shape, lambda i, s: (0, 0), pipeline_mode=pl.Buffered(1))]
            + [any_space] * (1 + len(carried)),
            out_specs=[
                any_space,
                pl.BlockSpec((cols, tile), lambda i, s: (0, start + i)),
                pl.BlockSpec(((h - 1) * cols, tile), lambda i, s: (0, i)),
            ],
            scratch_shapes=[
                pltpu.VMEM((tile, n * cols), jnp.bfloat16),
                pltpu.VMEM((tile, h * cols), jnp.bfloat16),
                pltpu.VMEM((rows, tile), jnp.bfloat16),
                pltpu.VMEM(ssq.shape, ssq.dtype),
                pltpu.VMEM((rows, h * cols), jnp.float32),
                pltpu.VMEM((rows, h * cols) if last else (8, 128), jnp.bfloat16),
                pltpu.SemaphoreType.DMA,
                pltpu.SemaphoreType.DMA,
            ],
        ),
        out_shape=[
            acc_shape,
            jax.ShapeDtypeStruct((cols, units), jnp.float32),
            jax.ShapeDtypeStruct(((h - 1) * cols, length), jnp.bfloat16),
        ],
        input_output_aliases=aliases,
        compiler_params=pltpu.CompilerParams(
            dimension_semantics=("arbitrary",), vmem_limit_bytes=VMEM
        ),
        cost_estimate=pl.CostEstimate(
            flops=2 * rows * length * cols * (n + 2 * h),
            bytes_accessed=8 * length * n * cols + 8 * rows * cols * (n + h),
            transcendentals=rows * length,
        ),
    )(where, *gate, *down, g_noise, d_noise, tok, ssq, *carried)


def merge_call(at_end, got, out, lo):
    rows, length = got.shape

    def body(flag, got_ref, _, out_ref, narrow, wide, sem):
        @pl.when(flag[0] == 1)
        def _():
            load = pltpu.make_async_copy(got_ref, narrow, sem)
            load.start()
            load.wait()
            wide[...] = narrow[...].astype(jnp.float32)
            store = pltpu.make_async_copy(wide, out_ref.at[:, pl.ds(lo, length)], sem)
            store.start()
            store.wait()

    any_space = pl.BlockSpec(memory_space=pl.ANY)
    return pl.pallas_call(
        body,
        in_specs=[pl.BlockSpec(memory_space=pltpu.SMEM), any_space, any_space],
        out_specs=any_space,
        scratch_shapes=[
            pltpu.VMEM((rows, length), got.dtype),
            pltpu.VMEM((rows, length), out.dtype),
            pltpu.SemaphoreType.DMA,
        ],
        out_shape=jax.ShapeDtypeStruct(out.shape, out.dtype),
        input_output_aliases={2: 0},
        cost_estimate=pl.CostEstimate(
            flops=2000000, bytes_accessed=6 * rows * length, transcendentals=0
        ),
    )(at_end, got, out)


def shard_step(
    tokens, cotangent, expert_ids, router_logits, gate_mean, down_mean, gate_noise, down_noise
):
    devices = lax.axis_size("expert")
    n = lax.axis_size("dp")
    h = n // 2
    slices = devices // E
    tok, width = tokens.shape
    units, cols = gate_mean.shape
    me = lax.axis_index("dp")
    right = me >= h
    is_mid = (me == h - 1) | (me == h)

    def same(x, p):
        return lax.ppermute(x, "dp", [(p, h - 1), (n - 1 - p, h)])

    def swap(x):
        return lax.ppermute(x, "dp", [(h - 1, h), (h, h - 1)])

    def cross(x, p):
        return lax.ppermute(x, "dp", [(p, h), (n - 1 - p, h - 1)])

    def back(x, p):
        return lax.ppermute(x, "dp", [(h - 1, p), (h, n - 1 - p)])

    def slice_at(p):
        return jnp.where(right, n - 1 - p, p)

    def cols_at(x, p):
        return lax.dynamic_slice_in_dim(x, slice_at(p) * cols, cols, axis=1)

    def gathered(near, far):
        got = [same(near, p) for p in range(h - 1)] + [near]
        return got + [cross(far, n - 1 - p) for p in range(h, n)]

    flat_ids = expert_ids.reshape(tok * TOPK)
    member = (flat_ids[:, None] == jnp.arange(E, dtype=jnp.int32)[None, :]).astype(jnp.int32)
    earlier = jnp.cumsum(member, axis=0) - member
    slot = jnp.sum(earlier * member, axis=1)
    rows_e = n * CAP
    target = (flat_ids * rows_e + me * CAP + slot).reshape(tok, TOPK)
    meta = jnp.concatenate([target.astype(jnp.float32), router_logits], axis=1)
    meta = jnp.concatenate(gathered(meta, meta), axis=0)
    target = meta[:, :TOPK].astype(jnp.int32)
    logits = meta[:, TOPK:]
    mixing = 1.0 / (1.0 + jnp.exp(logits[:, ::-1] - logits))

    def side_cols(x, of_right):
        return jnp.where(of_right, x[:, h * cols:], x[:, : h * cols])

    mine, other = side_cols(cotangent, right), side_cols(cotangent, ~right)
    load = jnp.concatenate(
        gathered(jnp.concatenate([tokens, mine], axis=1), jnp.concatenate([tokens, other], axis=1)),
        axis=0,
    )
    all_tok, all_cot = load[:, :width], load[:, width:]

    bounds = [0]
    for cut in CUTS:
        bounds.append(bounds[-1] + units * cut // sum(CUTS))
    chunks = list(zip(bounds[:-1], bounds[1:]))
    gate_parts, down_parts = [], []
    for lo, hi in chunks:
        piece = gate_mean[lo:hi]
        near = [same(piece, p) for p in range(h - 1)]
        far = [swap(piece)]
        far += [swap(near[q]) for q in range(h - 2, -1, -1)]
        gate_parts.append(near + [piece] + far)
        piece = down_mean[lo:hi]
        down_parts.append([same(piece, p) for p in range(h - 1)] + [piece])

    row_ids = jnp.arange(E * rows_e, dtype=jnp.int32)
    hits = [row_ids[:, None] == target[:, k][None, :] for k in range(TOPK)]
    placing = jnp.logical_or(hits[0], hits[1]).astype(jnp.bfloat16)
    flipped = jnp.concatenate([cols_at(all_tok, p) for p in range(n)], axis=1)
    token_out = jnp.dot(placing, flipped, preferred_element_type=jnp.float32).astype(jnp.bfloat16)
    half_cols = [all_cot[:, p * cols:(p + 1) * cols] for p in range(h)]
    ordered = jnp.concatenate(
        [jnp.where(right, half_cols[h - 1 - p], half_cols[p]) for p in range(h)], axis=1
    )
    scaled = [
        (mixing[:, k][:, None] * ordered.astype(jnp.float32)).astype(jnp.bfloat16)
        for k in range(TOPK)
    ]
    squares = [jnp.square(x.astype(jnp.float32)).astype(jnp.bfloat16) for x in scaled]
    scaled_sq = jnp.dot(
        jnp.concatenate(hits, axis=1).astype(jnp.bfloat16),
        jnp.concatenate(squares, axis=0),
        preferred_element_type=jnp.float32,
    ).astype(jnp.bfloat16)

    def to_experts(x):
        wide = x.shape[1]
        x = jnp.broadcast_to(x.reshape(E, 1, rows_e, wide), (E, slices, rows_e, wide))
        x = lax.all_to_all(
            x.reshape(devices, rows_e, wide), "expert", split_axis=0, concat_axis=0, tiled=True
        )
        return x.reshape(devices * rows_e, wide)

    token_rows = to_experts(token_out)
    ssq = to_experts(scaled_sq)

    factor = E / (tok * n * devices)
    if devices * rows_e <= 2048:
        where = jnp.stack([slice_at(p) for p in range(n)]).astype(jnp.int32)
        at_end = jnp.logical_not(is_mid).astype(jnp.int32).reshape(1)
        acc, precision = None, None
        ssq_t = ssq.T
        waiting = []

        def merge_one(precision):
            lo, sent = waiting.pop(0)
            got = sent[0]
            for p in range(1, h - 1):
                got = jnp.where((me == p) | (me == n - 1 - p), sent[p], got)
            return merge_call(at_end, got, precision, lo)

        for c, (lo, hi) in enumerate(chunks):
            acc, precision, sent = chunk_call(
                n, h, lo, hi - lo, units, factor, where, gate_parts[c], down_parts[c],
                gate_noise, down_noise, token_rows, ssq_t, acc, precision,
            )
            sent = [back(sent[p * cols:(p + 1) * cols], p) for p in range(h - 1)]
            waiting.append((lo, sent))
            if len(waiting) > 2 and h > 1:
                precision = merge_one(precision)
        while waiting and h > 1:
            precision = merge_one(precision)
        value = acc
    else:
        def joined(parts, count):
            return jnp.concatenate(
                [jnp.concatenate([x[p] for x in parts], axis=0) for p in range(count)], axis=1
            )

        def summed(parts, noise, count):
            noise = jnp.concatenate([cols_at(noise, p) for p in range(count)], axis=1)
            mean = joined(parts, count).astype(jnp.float32)
            return (mean + noise.astype(jnp.float32)).astype(jnp.bfloat16)

        pre = lax.dot_general(
            token_rows, summed(gate_parts, gate_noise, n), (((1,), (1,)), ((), ())),
            preferred_element_type=jnp.float32,
        )
        hidden = silu_of(pre).astype(jnp.bfloat16)
        value = jnp.dot(
            hidden, summed(down_parts, down_noise, h), preferred_element_type=jnp.float32
        ).astype(jnp.bfloat16)
        hidden_sq = jnp.square(hidden.astype(jnp.float32)).astype(jnp.bfloat16)
        prec = factor * lax.dot_general(
            ssq, hidden_sq, (((0,), (0,)), ((), ())), preferred_element_type=jnp.float32
        )
        precision = prec[(h - 1) * cols:]
        for p in range(h - 1):
            sent = back(prec[p * cols:(p + 1) * cols].astype(jnp.bfloat16), p)
            at_p = (me == p) | (me == n - 1 - p)
            precision = jnp.where(at_p, sent.astype(jnp.float32), precision)

    returned = lax.all_to_all(
        value.reshape(devices, rows_e, h * cols), "expert", split_axis=0, concat_axis=0, tiled=True
    )
    returned = returned.reshape(E, slices, rows_e, h * cols)
    if slices > 1:
        returned = jnp.sum(returned.astype(jnp.float32), axis=1)
        pick = jnp.float32
    else:
        pick = jnp.bfloat16
    returned = returned.reshape(E * rows_e, h * cols)
    combined = sum(
        mixing[:, k][:, None]
        * lax.dot_general(
            hits[k].astype(pick), returned, (((0,), (0,)), ((), ())),
            preferred_element_type=jnp.float32,
            precision=lax.Precision.HIGHEST if slices > 1 else None,
        )
        for k in range(TOPK)
    ).astype(jnp.bfloat16)
    parts = [combined[:, p * cols:(p + 1) * cols] for p in range(h)]
    combined = jnp.concatenate(
        [jnp.where(right, parts[h - 1 - p], parts[p]) for p in range(h)], axis=1
    )
    own = combined[(h - 1) * tok:h * tok]
    far = None
    for p in range(n):
        if p == h - 1:
            continue
        got = back(combined[p * tok:(p + 1) * tok], p)
        if p < h - 1:
            own = jnp.where((me == p) | (me == n - 1 - p), got, own)
        elif far is None:
            far = got
        else:
            far = jnp.where((me == p) | (me == n - 1 - p), got, far)
    mixed = jnp.concatenate(
        [jnp.where(right, far, own), jnp.where(right, own, far)], axis=1
    )
    return (mixed, precision)


def solution(mesh):
    return jax.shard_map(
        shard_step,
        mesh=mesh,
        in_specs=(
            P(("dp", "expert"), None),
            P(("dp", "expert"), None),
            P(("dp", "expert"), None),
            P(("dp", "expert"), None),
            P("expert", "dp"),
            P("expert", "dp"),
            P("expert", None),
            P("expert", None),
        ),
        out_specs=(P(("dp", "expert"), None), P("dp", "expert")),
        check_vma=False,
    )
```

```python
import jax
import jax.numpy as jnp
from jax import lax
from jax.experimental import pallas as pl
from jax.experimental.pallas import tpu as pltpu
from jax.sharding import PartitionSpec as P

E = 8
TOPK = 2
CAP = 36
CUTS = (4, 3, 3, 2, 2)
VMEM = 60 * 1024 * 1024
TILE = 512
BLOCKS = 3


def silu_of(values):
    return values / (1.0 + jnp.exp(-values))


def chunk_body(n, h, cols, blocks, factor, first, last, where_ref, *refs):
    gate = refs[:n]
    down = refs[n:n + h]
    g_noise, d_noise, tok_ref, ssq_ref = refs[n + h:n + h + 4]
    acc_in = None if first else refs[n + h + 4]
    refs = refs[n + h + (4 if first else 6):]
    acc_out, out, sent, w, dw, hsq, ssq, acc, held, acc_sem, ssq_sem = refs
    rows = tok_ref.shape[0] // blocks
    step = pl.program_id(0)
    busy = where_ref[n] == 1
    ssq_load = pltpu.make_async_copy(ssq_ref, ssq, ssq_sem)
    if not first:
        acc_load = pltpu.make_async_copy(acc_in, acc, acc_sem)
    if last:
        acc_store = pltpu.make_async_copy(held, acc_out, acc_sem)
    else:
        acc_store = pltpu.make_async_copy(acc, acc_out, acc_sem)
    opens = step == 0
    closes = step == pl.num_programs(0) - 1

    @pl.when(busy & opens)
    def _():
        if first:
            acc[...] = jnp.zeros_like(acc)
        else:
            acc_load.start()
        ssq_load.start()

    @pl.when(busy)
    def _():
        for p in range(n):
            at = pl.ds(pl.multiple_of(where_ref[p] * cols, cols), cols)
            w[:, p * cols:(p + 1) * cols] = gate[p][...] + g_noise[:, at]
            if p < h:
                near = where_ref[p] - where_ref[n + 1] * h
                at = pl.ds(pl.multiple_of(near * cols, cols), cols)
                dw[:, p * cols:(p + 1) * cols] = down[p][...] + d_noise[:, at]

    if not first:
        @pl.when(busy & opens)
        def _():
            acc_load.wait()

    @pl.when(busy)
    def _():
        def some_rows(r, carry):
            at = pl.ds(pl.multiple_of(r * rows, rows), rows)
            pre = lax.dot_general(
                tok_ref[at, :], w[...], (((1,), (1,)), ((), ())),
                preferred_element_type=jnp.float32,
            )
            hidden = silu_of(pre).astype(jnp.bfloat16)
            hsq[at, :] = jnp.square(hidden.astype(jnp.float32)).astype(jnp.bfloat16)
            acc[at, :] += jnp.dot(hidden, dw[...], preferred_element_type=jnp.float32)
            return carry

        lax.fori_loop(0, blocks, some_rows, 0)

    @pl.when(busy & closes)
    def _():
        if last:
            held[...] = acc[...].astype(held.dtype)
        acc_store.start()

    @pl.when(busy & opens)
    def _():
        ssq_load.wait()

    @pl.when(busy)
    def _():
        sent[...] = (
            factor
            * jnp.dot(ssq[: (h - 1) * cols, :], hsq[...], preferred_element_type=jnp.float32)
        ).astype(jnp.bfloat16)
        out[...] = factor * jnp.dot(
            ssq[(h - 1) * cols:, :], hsq[...], preferred_element_type=jnp.float32
        )

    @pl.when(busy & closes)
    def _():
        acc_store.wait()


def chunk_call(
    n, h, lo, length, units, factor, where, gate, down, g_noise, d_noise, tok, ssq, acc, out
):
    cols = gate[0].shape[1]
    rows = tok.shape[0]
    first, last = acc is None, lo + length == units
    tile = TILE if length % TILE == 0 else length
    start = lo // tile
    blocks = BLOCKS if rows % (8 * BLOCKS) == 0 else 1
    mean_spec = pl.BlockSpec((tile, cols), lambda i, s: (i, 0))
    noise_spec = pl.BlockSpec((tile, n * cols), lambda i, s: (start + i, 0))
    side_spec = pl.BlockSpec((tile, h * cols), lambda i, s: (start + i, s[n + 1]))
    any_space = pl.BlockSpec(memory_space=pl.ANY)
    acc_shape = jax.ShapeDtypeStruct((rows, h * cols), jnp.bfloat16 if last else jnp.float32)
    carried = () if first else (acc, out)
    aliases = {} if first else {n + h + 6: 1}
    if not (first or last):
        aliases[n + h + 5] = 0

    def kernel(*refs):
        return chunk_body(n, h, cols, blocks, factor, first, last, *refs)

    return pl.pallas_call(
        kernel,
        grid_spec=pltpu.PrefetchScalarGridSpec(
            num_scalar_prefetch=1,
            grid=(length // tile,),
            in_specs=[mean_spec] * (n + h)
            + [noise_spec, side_spec]
            + [pl.BlockSpec(tok.shape, lambda i, s: (0, 0), pipeline_mode=pl.Buffered(1))]
            + [any_space] * (1 + len(carried)),
            out_specs=[
                any_space,
                pl.BlockSpec((cols, tile), lambda i, s: (0, start + i)),
                pl.BlockSpec(((h - 1) * cols, tile), lambda i, s: (0, i)),
            ],
            scratch_shapes=[
                pltpu.VMEM((tile, n * cols), jnp.bfloat16),
                pltpu.VMEM((tile, h * cols), jnp.bfloat16),
                pltpu.VMEM((rows, tile), jnp.bfloat16),
                pltpu.VMEM(ssq.shape, ssq.dtype),
                pltpu.VMEM((rows, h * cols), jnp.float32),
                pltpu.VMEM((rows, h * cols) if last else (8, 128), jnp.bfloat16),
                pltpu.SemaphoreType.DMA,
                pltpu.SemaphoreType.DMA,
            ],
        ),
        out_shape=[
            acc_shape,
            jax.ShapeDtypeStruct((cols, units), jnp.float32),
            jax.ShapeDtypeStruct(((h - 1) * cols, length), jnp.bfloat16),
        ],
        input_output_aliases=aliases,
        compiler_params=pltpu.CompilerParams(
            dimension_semantics=("arbitrary",), vmem_limit_bytes=VMEM
        ),
        cost_estimate=pl.CostEstimate(
            flops=2 * rows * length * cols * (n + 2 * h),
            bytes_accessed=8 * length * n * cols + 8 * rows * cols * (n + h),
            transcendentals=rows * length,
        ),
    )(where, *gate, *down, g_noise, d_noise, tok, ssq, *carried)


def merge_call(at_end, got, out, lo):
    rows, length = got.shape

    def body(flag, got_ref, _, out_ref, narrow, wide, sem):
        @pl.when(flag[0] == 1)
        def _():
            load = pltpu.make_async_copy(got_ref, narrow, sem)
            load.start()
            load.wait()

            def some(r, carry):
                at = pl.ds(pl.multiple_of(r * 32, 32), 32)
                wide[at, :] = narrow[at, :].astype(jnp.float32)
                return carry

            lax.fori_loop(0, rows // 32, some, 0)
            store = pltpu.make_async_copy(wide, out_ref.at[:, pl.ds(lo, length)], sem)
            store.start()
            store.wait()

    any_space = pl.BlockSpec(memory_space=pl.ANY)
    return pl.pallas_call(
        body,
        in_specs=[pl.BlockSpec(memory_space=pltpu.SMEM), any_space, any_space],
        out_specs=any_space,
        scratch_shapes=[
            pltpu.VMEM((rows, length), got.dtype),
            pltpu.VMEM((rows, length), out.dtype),
            pltpu.SemaphoreType.DMA,
        ],
        out_shape=jax.ShapeDtypeStruct(out.shape, out.dtype),
        input_output_aliases={2: 0},
        cost_estimate=pl.CostEstimate(
            flops=2000000, bytes_accessed=6 * rows * length, transcendentals=0
        ),
    )(at_end, got, out)


def shard_step(
    tokens, cotangent, expert_ids, router_logits, gate_mean, down_mean, gate_noise, down_noise
):
    devices = lax.axis_size("expert")
    n = lax.axis_size("dp")
    h = n // 2
    slices = devices // E
    tok, _ = tokens.shape
    units, cols = gate_mean.shape
    me = lax.axis_index("dp")
    right = me >= h
    is_mid = (me == h - 1) | (me == h)

    def same(x, p):
        return lax.ppermute(x, "dp", [(p, h - 1), (n - 1 - p, h)])

    def swap(x):
        return lax.ppermute(x, "dp", [(h - 1, h), (h, h - 1)])

    def cross(x, p):
        return lax.ppermute(x, "dp", [(p, h), (n - 1 - p, h - 1)])

    def back(x, p):
        return lax.ppermute(x, "dp", [(h - 1, p), (h, n - 1 - p)])

    def slice_at(p):
        return jnp.where(right, n - 1 - p, p)

    def cols_at(x, p):
        return lax.dynamic_slice_in_dim(x, slice_at(p) * cols, cols, axis=1)

    def gathered(near, far):
        got = [same(near, p) for p in range(h - 1)] + [near]
        return got + [cross(far, n - 1 - p) for p in range(h, n)]

    flat_ids = expert_ids.reshape(tok * TOPK)
    member = (flat_ids[:, None] == jnp.arange(E, dtype=jnp.int32)[None, :]).astype(jnp.int32)
    earlier = jnp.cumsum(member, axis=0) - member
    slot = jnp.sum(earlier * member, axis=1)
    rows_e = n * CAP
    target = (flat_ids * rows_e + me * CAP + slot).reshape(tok, TOPK)
    meta = jnp.concatenate([target.astype(jnp.float32), router_logits], axis=1)
    meta = jnp.concatenate(gathered(meta, meta), axis=0)
    target = meta[:, :TOPK].astype(jnp.int32)
    logits = meta[:, TOPK:]
    mixing = 1.0 / (1.0 + jnp.exp(logits[:, ::-1] - logits))

    def side_cols(x, of_right):
        return jnp.where(of_right, x[:, h * cols:], x[:, : h * cols])

    mine, other = side_cols(cotangent, right), side_cols(cotangent, ~right)
    all_tok = jnp.concatenate(gathered(tokens, tokens), axis=0)
    all_cot = jnp.concatenate(gathered(mine, other), axis=0)

    bounds = [0]
    for cut in CUTS:
        bounds.append(bounds[-1] + units * cut // sum(CUTS))
    chunks = list(zip(bounds[:-1], bounds[1:]))
    gate_parts, down_parts = [], []
    for lo, hi in chunks:
        piece = gate_mean[lo:hi]
        near = [same(piece, p) for p in range(h - 1)]
        far = [swap(piece)]
        far += [swap(near[q]) for q in range(h - 2, -1, -1)]
        gate_parts.append(near + [piece] + far)
        piece = down_mean[lo:hi]
        down_parts.append([same(piece, p) for p in range(h - 1)] + [piece])

    row_ids = jnp.arange(E * rows_e, dtype=jnp.int32)
    hits = [row_ids[:, None] == target[:, k][None, :] for k in range(TOPK)]
    placing = jnp.logical_or(hits[0], hits[1]).astype(jnp.bfloat16)
    flipped = jnp.concatenate([cols_at(all_tok, p) for p in range(n)], axis=1)
    token_out = jnp.dot(placing, flipped, preferred_element_type=jnp.float32).astype(jnp.bfloat16)
    half_cols = [all_cot[:, p * cols:(p + 1) * cols] for p in range(h)]
    ordered = jnp.concatenate(
        [jnp.where(right, half_cols[h - 1 - p], half_cols[p]) for p in range(h)], axis=1
    )
    scaled = [
        (mixing[:, k][:, None] * ordered.astype(jnp.float32)).astype(jnp.bfloat16)
        for k in range(TOPK)
    ]
    squares = [jnp.square(x.astype(jnp.float32)).astype(jnp.bfloat16) for x in scaled]
    scaled_sq = jnp.dot(
        jnp.concatenate(hits, axis=1).astype(jnp.bfloat16),
        jnp.concatenate(squares, axis=0),
        preferred_element_type=jnp.float32,
    ).astype(jnp.bfloat16)

    def to_experts(x):
        wide = x.shape[1]
        x = jnp.broadcast_to(x.reshape(E, 1, rows_e, wide), (E, slices, rows_e, wide))
        x = lax.all_to_all(
            x.reshape(devices, rows_e, wide), "expert", split_axis=0, concat_axis=0, tiled=True
        )
        return x.reshape(devices * rows_e, wide)

    token_rows = to_experts(token_out)
    ssq = to_experts(scaled_sq)

    factor = E / (tok * n * devices)
    if devices * rows_e <= 2048:
        where = jnp.stack([slice_at(p) for p in range(n)] + [is_mid, right]).astype(jnp.int32)
        at_end = jnp.logical_not(is_mid).astype(jnp.int32).reshape(1)
        acc, precision = None, None
        ssq_t = ssq.T
        waiting = []

        def merge_one(precision):
            lo, sent = waiting.pop(0)
            got = sent[0]
            for p in range(1, h - 1):
                got = jnp.where((me == p) | (me == n - 1 - p), sent[p], got)
            return merge_call(at_end, got, precision, lo)

        for c, (lo, hi) in enumerate(chunks):
            acc, precision, sent = chunk_call(
                n, h, lo, hi - lo, units, factor, where, gate_parts[c], down_parts[c],
                gate_noise, down_noise, token_rows, ssq_t, acc, precision,
            )
            sent = [back(sent[p * cols:(p + 1) * cols], p) for p in range(h - 1)]
            waiting.append((lo, sent))
            if len(waiting) > 2 and h > 1:
                precision = merge_one(precision)
        while waiting and h > 1:
            precision = merge_one(precision)
        value = acc
    else:
        def joined(parts, count):
            return jnp.concatenate(
                [jnp.concatenate([x[p] for x in parts], axis=0) for p in range(count)], axis=1
            )

        def summed(parts, noise, count):
            noise = jnp.concatenate([cols_at(noise, p) for p in range(count)], axis=1)
            mean = joined(parts, count).astype(jnp.float32)
            return (mean + noise.astype(jnp.float32)).astype(jnp.bfloat16)

        pre = lax.dot_general(
            token_rows, summed(gate_parts, gate_noise, n), (((1,), (1,)), ((), ())),
            preferred_element_type=jnp.float32,
        )
        hidden = silu_of(pre).astype(jnp.bfloat16)
        value = jnp.dot(
            hidden, summed(down_parts, down_noise, h), preferred_element_type=jnp.float32
        ).astype(jnp.bfloat16)
        hidden_sq = jnp.square(hidden.astype(jnp.float32)).astype(jnp.bfloat16)
        prec = factor * lax.dot_general(
            ssq, hidden_sq, (((0,), (0,)), ((), ())), preferred_element_type=jnp.float32
        )
        precision = prec[(h - 1) * cols:]
        for p in range(h - 1):
            sent = back(prec[p * cols:(p + 1) * cols].astype(jnp.bfloat16), p)
            at_p = (me == p) | (me == n - 1 - p)
            precision = jnp.where(at_p, sent.astype(jnp.float32), precision)

    returned = lax.all_to_all(
        value.reshape(devices, rows_e, h * cols), "expert", split_axis=0, concat_axis=0, tiled=True
    )
    returned = returned.reshape(E, slices, rows_e, h * cols)
    if slices > 1:
        returned = jnp.sum(returned.astype(jnp.float32), axis=1)
        pick = jnp.float32
    else:
        pick = jnp.bfloat16
    returned = returned.reshape(E * rows_e, h * cols)
    combined = sum(
        mixing[:, k][:, None]
        * lax.dot_general(
            hits[k].astype(pick), returned, (((0,), (0,)), ((), ())),
            preferred_element_type=jnp.float32,
            precision=lax.Precision.HIGHEST if slices > 1 else None,
        )
        for k in range(TOPK)
    ).astype(jnp.bfloat16)
    parts = [combined[:, p * cols:(p + 1) * cols] for p in range(h)]
    combined = jnp.concatenate(
        [jnp.where(right, parts[h - 1 - p], parts[p]) for p in range(h)], axis=1
    )
    own = combined[(h - 1) * tok:h * tok]
    far = None
    for p in range(n):
        if p == h - 1:
            continue
        got = back(combined[p * tok:(p + 1) * tok], p)
        if p < h - 1:
            own = jnp.where((me == p) | (me == n - 1 - p), got, own)
        elif far is None:
            far = got
        else:
            far = jnp.where((me == p) | (me == n - 1 - p), got, far)
    mixed = jnp.concatenate(
        [jnp.where(right, far, own), jnp.where(right, own, far)], axis=1
    )
    return (mixed, precision)


def solution(mesh):
    return jax.shard_map(
        shard_step,
        mesh=mesh,
        in_specs=(
            P(("dp", "expert"), None),
            P(("dp", "expert"), None),
            P(("dp", "expert"), None),
            P(("dp", "expert"), None),
            P("expert", "dp"),
            P("expert", "dp"),
            P("expert", None),
            P("expert", None),
        ),
        out_specs=(P(("dp", "expert"), None), P("dp", "expert")),
        check_vma=False,
    )
```
